256 devices in a mesh: img: 16 (over x, z_lo, core), tp: 16 (over y, z_hi).
Axes of the slice: x: 4, y: 4, z: 8 (z_hi: 4, z_lo: 2; z = z_hi * 2 + z_lo), core: 2. Of those that a mesh axis runs over, the one named last changes fastest.
Arguments:
- patch_tokens: bfloat16 [32768, 1024], P(('img', 'tp')), may hold values from -12 to 12
- norm_gain: float32 [1024], replicated, may hold values from 0.1 to 1.9
- norm_bias: float32 [1024], replicated, may hold values from -3 to 3
- up_weight: bfloat16 [1024, 8192], P('img', 'tp'), may hold values from -0.1875 to 0.1875
- up_bias: float32 [8192], P('tp'), may hold values from -3 to 3
- down_weight: bfloat16 [8192, 4096], P('tp', 'img'), may hold values from -0.125 to 0.125
- down_bias: float32 [4096], replicated, may hold values from -3 to 3
Outputs:
- projected: bfloat16 [32768, 4096], P(('img', 'tp'))
The draws below stay inside these ranges and needn't reach their ends.
All inputs are finite; a program needn't handle non-finite values.
Results may differ from the reference program's by a relative error of at most 0.014.
Values may be sent and summed in bfloat16 or wider, within the bound.
No kernel may reach another device: no remote copies, remote signals or barrier semaphores. Data moves between devices by JAX's collectives and lax.ppermute only.
A program may use at most 128 MiB of HBM per device.

```python
import jax
import jax.numpy as jnp
from jax import lax

D = 1024
FF = 8192
DOUT = 4096
TOK_DEV = 128
TOKENS = 32768
N_IMG = 16
N_TP = 16


def level_of(own_key, dims, pieces, low, top_value):
    loudness = 1.0
    for axis_at, blocks in pieces:
        draws = jax.random.uniform(jax.random.fold_in(jax.random.fold_in(own_key, 6), axis_at), (blocks,), jnp.float32, low / len(pieces), top_value / len(pieces))
        loudness = loudness * jnp.repeat(jnp.exp(draws), dims[axis_at] // blocks).reshape((-1,) + (1,) * (len(dims) - 1 - axis_at))
    return loudness


def centred(rng, dims, width, reach, pieces=(), held_as=jnp.bfloat16):
    result = width * jax.random.normal(rng, dims, jnp.float32)
    if pieces:
        result = result * level_of(rng, dims, pieces, -0.22, 0.18)
    return jnp.clip(result, -reach, reach).astype(held_as)


def setup_inputs(seed: int = 0) -> dict:
    keys = jax.random.split(jax.random.key(seed), 8)
    patch_tokens = centred(keys[0], (TOKENS, D), 2.0, 12.0, ((0, 256),))
    norm_gain = jnp.clip(1.0 + 0.18 * jax.random.normal(keys[1], (D,), jnp.float32), 0.1, 1.9)
    norm_bias = centred(keys[2], (D,), 0.5, 3.0, (), jnp.float32)
    up_weight = centred(keys[3], (D, FF), D ** -0.5, 0.1875, ((0, 16), (1, 16)))
    up_bias = centred(keys[4], (FF,), 0.5, 3.0, ((0, 16),), jnp.float32)
    down_weight = centred(keys[5], (FF, DOUT), (FF // 4) ** -0.5, 0.125, ((0, 16), (1, 16)))
    down_bias = centred(keys[6], (DOUT,), 0.5, 3.0, (), jnp.float32)
    return dict(patch_tokens=patch_tokens, norm_gain=norm_gain, norm_bias=norm_bias, up_weight=up_weight, up_bias=up_bias, down_weight=down_weight, down_bias=down_bias)


def normalize(rows, norm_gain, norm_bias):
    values = rows.astype(jnp.float32)
    center = lax.optimization_barrier(jnp.mean(values, axis=1, keepdims=True))
    spread = lax.optimization_barrier(jnp.mean((values - center) ** 2, axis=1, keepdims=True))
    return ((values - center) * lax.rsqrt(spread + 1e-05) * norm_gain + norm_bias).astype(jnp.bfloat16)

def reference(patch_tokens, norm_gain, norm_bias, up_weight, up_bias, down_weight, down_bias):
    block_rows = TOK_DEV * N_TP
    group_width = FF // N_TP
    blocks = patch_tokens.reshape(N_IMG, block_rows, D)

    def one_block(rows):
        normed = normalize(rows, norm_gain, norm_bias)
        hidden = jax.nn.gelu(jnp.dot(normed, up_weight, preferred_element_type=jnp.float32) + up_bias).astype(jnp.bfloat16)

        def add_group(group, total):
            start = (group * group_width).astype(jnp.int32)
            cols = lax.dynamic_slice_in_dim(hidden, start, group_width, 1)
            weights = lax.dynamic_slice_in_dim(down_weight, start, group_width, 0)
            partial_value = jnp.dot(cols, weights, preferred_element_type=jnp.float32).astype(jnp.bfloat16)
            partial_value = lax.optimization_barrier(partial_value)
            return total + partial_value.astype(jnp.float32)
        total = lax.fori_loop(0, N_TP, add_group, jnp.zeros((block_rows, DOUT), jnp.float32))
        return (total + down_bias).astype(jnp.bfloat16)
    return lax.map(one_block, blocks).reshape(TOKENS, DOUT)
```

```python
import functools

import jax
import jax.numpy as jnp
from jax import lax
from jax.experimental import pallas as pl
from jax.experimental.pallas import tpu as pltpu
from jax.sharding import Mesh
from jax.sharding import PartitionSpec as P

BF = jnp.bfloat16
F32 = jnp.float32
D, TOK = 1024, 128
X, Y, Z, ZH = 4, 4, 8, 4
GROUP = 512
COLS = 256
HID = ZH * GROUP
NX = 4 * COLS
ANY = pl.BlockSpec(memory_space=pl.ANY)
VMEM = pl.BlockSpec(memory_space=pltpu.VMEM)


def ring(n, d):
    return [(i, (i + d) % n) for i in range(n)]


def both_ways(n):
    return [(2 * i + c, 2 * ((i + (1 - 2 * c)) % n) + c) for i in range(n) for c in (0, 1)]


def on_x(a, d):
    return lax.ppermute(a, "x", ring(X, d))


def on_y(a, d):
    return lax.ppermute(a, "y", ring(Y, d))


def on_z(a):
    def at(i):
        return (i // 2 % 2 * 2 + i % 2) * ZH + i // 4

    return lax.ppermute(a, ("zl", "c", "zh"), [(at(i), at(j)) for i, j in both_ways(Z)])


def on_xc(a):
    return lax.ppermute(a, ("x", "c"), both_ways(X))


def on_c(a):
    return lax.ppermute(a, "c", [(0, 1), (1, 0)])


def norm_kernel(x_ref, g_ref, b_ref, o_ref):
    v = x_ref[...].astype(F32)
    center = jnp.mean(v, axis=1, keepdims=True)
    w = v - center
    spread = jnp.mean(w * w, axis=1, keepdims=True)
    o_ref[...] = (w * lax.rsqrt(spread + 1e-05) * g_ref[...] + b_ref[...]).astype(BF)


def normalize(rows, gain, bias):
    return pl.pallas_call(
        norm_kernel,
        out_shape=jax.ShapeDtypeStruct(rows.shape, BF),
        in_specs=[VMEM] * 3,
        out_specs=VMEM,
        name="norm",
        cost_estimate=pl.CostEstimate(flops=10**6, bytes_accessed=2**19, transcendentals=128),
    )(rows, gain[None], bias[None])


def side(c):
    return 2 * c - 1


def place_kernel(n_up, *refs):
    ups, downs = refs[:n_up], refs[n_up:-3]
    up_out, down_out, sem = refs[-3:]
    x, c = lax.axis_index("x"), lax.axis_index("c")
    z = lax.axis_index("zh") * 2 + lax.axis_index("zl")
    o = 1 - c

    def units(k):
        out = [(z, k)]
        for s in (1, 2, 3):
            zs = lax.rem(z + s * side(k) + Z, Z)
            out += [(zs, k), (zs, 1 - k)]
        return out + [(lax.rem(z + 4, Z), k)]

    def xs(d):
        return lax.rem(x + d + X, X)

    copies = []

    def copy(src, dst):
        cp = pltpu.make_async_copy(src, dst, sem)
        cp.start()
        copies.append(cp)

    where = [
        (x, c), (x, o),
        (xs(side(c)), c), (xs(side(c)), o),
        (xs(side(o)), o), (xs(side(o)), c),
        (xs(2), c), (xs(2), o),
    ]
    for ref, (xx, k) in zip(ups, where):
        for i, (zz, cc) in enumerate(units(k)):
            row = pl.multiple_of(((xx * 2 + lax.rem(zz, 2)) * 2 + cc) * 64, 64)
            copy(ref.at[pl.ds(i * 64, 64)], up_out.at[lax.div(zz, 2), pl.ds(row, 64)])

    def put(src, zz, cc):
        row = pl.multiple_of(lax.div(zz, 2) * GROUP, GROUP)
        copy(src, down_out.at[lax.rem(zz, 2) * 2 + cc, pl.ds(row, GROUP)])

    d0, e0 = downs[:2]
    put(d0, z, c)
    put(e0, z, o)
    for s in (1, 2, 3):
        w, e = downs[2 * s], downs[2 * s + 1]
        zs, zo = lax.rem(z + s * side(c) + Z, Z), lax.rem(z + s * side(o) + Z, Z)
        put(w.at[0], zs, c)
        put(w.at[1], zs, o)
        put(e.at[0], zo, o)
        put(e.at[1], zo, c)
    put(downs[8], lax.rem(z + 4, Z), c)
    put(downs[9], lax.rem(z + 4, Z), o)
    for cp in copies:
        cp.wait()


def place(ups, downs):
    return pl.pallas_call(
        functools.partial(place_kernel, len(ups)),
        out_shape=(
            jax.ShapeDtypeStruct((ZH, D, GROUP), BF),
            jax.ShapeDtypeStruct((4, HID, COLS), BF),
        ),
        in_specs=[ANY] * (len(ups) + len(downs)),
        out_specs=(VMEM, VMEM),
        scratch_shapes=[pltpu.SemaphoreType.DMA],
        compiler_params=pltpu.CompilerParams(vmem_limit_bytes=24 * 2**20),
        name="place",
        cost_estimate=pl.CostEstimate(flops=4 * 10**9, bytes_accessed=2**24, transcendentals=0),
    )(*ups, *downs)


def mlp_kernel(n_tok, *refs):
    toks, (up, bias, down), outs, (t_ref, h_ref) = (
        refs[:n_tok], refs[n_tok : n_tok + 3], refs[n_tok + 3 : -2], refs[-2:],
    )
    at = 0
    for t in toks:
        t_ref[at : at + t.shape[0]] = t[...]
        at += t.shape[0]

    @pl.loop(0, at // 256)
    def _(i):
        rows = pl.ds(pl.multiple_of(i * 256, 256), 256)
        for g in range(ZH):
            s = jnp.dot(t_ref[rows], up[g], preferred_element_type=F32) + bias[g : g + 1]
            h_ref[:, g * GROUP : (g + 1) * GROUP] = jax.nn.gelu(s).astype(BF)
        for j in range(4):
            o = jnp.dot(h_ref[...], down[j], preferred_element_type=F32)
            outs[j // 2][j % 2, rows] = o.astype(BF)


def mlp(toks, up, bias, down):
    rows = sum(t.shape[0] for t in toks)
    half = jax.ShapeDtypeStruct((2, rows, COLS), BF)
    return pl.pallas_call(
        functools.partial(mlp_kernel, len(toks)),
        out_shape=(half, half),
        in_specs=[VMEM] * (len(toks) + 3),
        out_specs=(VMEM, VMEM),
        scratch_shapes=[pltpu.VMEM((rows, D), BF), pltpu.VMEM((256, HID), BF)],
        compiler_params=pltpu.CompilerParams(vmem_limit_bytes=40 * 2**20),
        name="mlp",
        cost_estimate=pl.CostEstimate(
            flops=2 * rows * (D * HID + HID * NX), bytes_accessed=2**23, transcendentals=rows * HID
        ),
    )(*toks, up, bias, down)


def out_kernel(*refs):
    pieces, o_ref, sem = refs[:-2], refs[-2], refs[-1]
    x = lax.axis_index("x")
    copies = []
    for i, ref in enumerate(pieces):
        h, r = divmod(i, 4)
        xx = lax.rem(x + (0, X - 1, 1, 2)[r], X)
        for j in range(2):
            col = pl.multiple_of(xx * NX + h * 512 + j * 256, 256)
            cp = pltpu.make_async_copy(ref.at[j], o_ref.at[:, pl.ds(col, COLS)], sem)
            cp.start()
            copies.append(cp)
    for cp in copies:
        cp.wait()


def put_out(pieces):
    return pl.pallas_call(
        out_kernel,
        out_shape=jax.ShapeDtypeStruct((TOK, X * NX), BF),
        in_specs=[VMEM] * len(pieces),
        out_specs=ANY,
        scratch_shapes=[pltpu.SemaphoreType.DMA],
        name="put_out",
    )(*pieces)


def on_device(patch_tokens, norm_gain, norm_bias, up_weight, up_bias, down_weight, down_bias):
    u_pair = jnp.concatenate([up_weight, on_c(up_weight)], axis=0)
    u = [u_pair]
    for _ in range(3):
        u.append(on_z(u[-1]))
    u4 = on_z(u[3][:64])
    f = jnp.concatenate([up_weight, u[1], u[2], u[3], u4], axis=0)
    g = on_c(f)
    x1f, x1g = on_xc(f), on_xc(g)
    x2f = on_xc(x1f)
    ups = [f, g, x1f, x1g, on_c(x1f), on_c(x1g), x2f, on_c(x2f)]

    d_other = on_c(down_weight)
    w = [jnp.stack([down_weight, d_other])]
    for _ in range(3):
        w.append(on_z(w[-1]))
    w4 = on_z(w[3][0])
    downs = [down_weight, d_other]
    for a in w[1:]:
        downs += [a, on_c(a)]
    downs += [w4, on_c(w4)]

    zh = lax.axis_index("zh")
    biases = [up_bias] + [lax.ppermute(up_bias, "zh", ring(ZH, -d)) for d in (1, 2, 3)]
    bias = jnp.roll(jnp.stack(biases), zh, axis=0)

    own = normalize(patch_tokens, norm_gain, norm_bias)
    left, right = on_x(own, 1), on_x(own, -1)
    across = [on_x(left[:64], 1), on_x(right[64:], -1)]
    rest = jnp.concatenate([left, right, *across], axis=0)
    below = [on_y(own, 1), on_y(rest, 1)]
    above = [on_y(own, -1), on_y(rest, -1)]
    far = [
        on_y(below[0][:64], 1), on_y(above[0][64:], -1),
        on_y(below[1][:192], 1), on_y(above[1][192:], -1),
    ]

    up, down = place(ups, downs)
    p_far = mlp(far, up, bias, down)
    from_below = [on_y(p_far[h][0], 1) for h in range(2)]
    from_above = [on_y(p_far[h][1], -1) for h in range(2)]
    p_above = mlp(above, up, bias, down)
    p_below = mlp(below, up, bias, down)
    p_own = mlp([own, rest], up, bias, down)
    x = lax.axis_index("x")
    my_bias = lax.dynamic_slice(down_bias, (x * NX,), (NX,)).reshape(2, 2, 1, COLS)
    pieces = []
    for h in range(2):
        to_above = jnp.stack(
            [(p_above[h][0].astype(F32) + from_below[h].astype(F32)).astype(BF), p_above[h][1]]
        )
        to_below = jnp.stack(
            [p_below[h][0], (p_below[h][1].astype(F32) + from_above[h].astype(F32)).astype(BF)]
        )
        got_below, got_above = on_y(to_above, 1), on_y(to_below, -1)
        total = p_own[h].astype(F32) + got_below.astype(F32) + got_above.astype(F32)
        total = (total + my_bias[h]).astype(BF)
        pieces += [
            total[:, :128],
            on_x(total[:, 256:384], 1),
            on_x(total[:, 128:256], -1),
            on_x(total[:, 384:], 2),
        ]
    return put_out(pieces)


def solution(mesh):
    grid = Mesh(mesh.devices.reshape(X, 2, 2, Y, ZH), ("x", "zl", "c", "y", "zh"))
    img, tp = ("x", "zl", "c"), ("y", "zh")
    return jax.shard_map(
        on_device,
        mesh=grid,
        in_specs=(P((*img, *tp), None), P(), P(), P(img, tp), P(tp), P(tp, img), P()),
        out_specs=P((*img, *tp), None),
        check_vma=False,
    )
```

```python
import functools

import jax
import jax.numpy as jnp
from jax import lax
from jax.experimental import pallas as pl
from jax.experimental.pallas import tpu as pltpu
from jax.sharding import Mesh
from jax.sharding import PartitionSpec as P


BF = jnp.bfloat16
F32 = jnp.float32
D, TOK = 1024, 128
X, Y, Z, ZH = 4, 4, 8, 4
GROUP = 512
COLS = 256
HID = ZH * GROUP
NX = 4 * COLS
ANY = pl.BlockSpec(memory_space=pl.ANY)
VMEM = pl.BlockSpec(memory_space=pltpu.VMEM)


def ring(n, d):
    return [(i, (i + d) % n) for i in range(n)]


def both_ways(n, d=1):
    return [(2 * i + c, 2 * ((i + d - 2 * d * c) % n) + c) for i in range(n) for c in (0, 1)]


def on_x(a, d):
    return lax.ppermute(a, "x", ring(X, d))


def on_y(a, d):
    return lax.ppermute(a, "y", ring(Y, d))


def on_z(a, d):
    def at(i):
        return (i // 2 % 2 * 2 + i % 2) * ZH + i // 4

    return lax.ppermute(a, ("zl", "c", "zh"), [(at(i), at(j)) for i, j in both_ways(Z, d)])


def on_xc(a):
    return lax.ppermute(a, ("x", "c"), both_ways(X))


def on_c(a):
    return lax.ppermute(a, "c", [(0, 1), (1, 0)])


def norm_kernel(x_ref, g_ref, b_ref, o_ref):
    v = x_ref[...].astype(F32)
    center = jnp.mean(v, axis=1, keepdims=True)
    w = v - center
    spread = jnp.mean(w * w, axis=1, keepdims=True)
    o_ref[...] = (w * lax.rsqrt(spread + 1e-05) * g_ref[...] + b_ref[...]).astype(BF)


def normalize(rows, gain, bias):
    return pl.pallas_call(
        norm_kernel,
        out_shape=jax.ShapeDtypeStruct(rows.shape, BF),
        in_specs=[VMEM] * 3,
        out_specs=VMEM,
        compiler_params=pltpu.CompilerParams(vmem_limit_bytes=8 * 2**20),
        name="norm",
        cost_estimate=pl.CostEstimate(flops=10**6, bytes_accessed=2**19, transcendentals=128),
    )(rows, gain[None], bias[None])


def side(c):
    return 2 * c - 1


UP_EARLY, UP_LATE = ("f", "g", "x1f", "x1g", "ex1f"), ("ex1g", "x2f", "ex2f")
DOWN_EARLY, DOWN_LATE = ("w0", "e0", "w1", "w2", "e1", "e2", "w3"), ("e3", "w4", "e4")
BIASES = ("w0", "w1", "w2", "w3", "w4", "e1", "e2", "e3", "e4")


def place_kernel(ups, downs, biases, n_old, *refs):
    n = len(ups) + len(downs) + len(biases)
    pieces = dict(zip(ups + downs + biases, refs))
    up_out, down_out, *bias_out, part, sem = refs[n + n_old :]
    x, c = lax.axis_index("x"), lax.axis_index("c")
    z = lax.axis_index("zh") * 2 + lax.axis_index("zl")
    o = 1 - c
    copies = []

    def copy(src, dst):
        cp = pltpu.make_async_copy(src, dst, sem)
        cp.start()
        copies.append(cp)

    def xs(d):
        return lax.rem(x + d + X, X)

    def put(src, zz, cc):
        row = pl.multiple_of(lax.div(zz, 2) * GROUP, GROUP)
        copy(src, down_out.at[lax.rem(zz, 2) * 2 + cc, pl.ds(row, GROUP)])

    def source(name):
        s, k = int(name[1]), c if name[0] == "w" else o
        return pieces[name], s, k, lax.rem(z + s * side(k) + Z, Z)

    for name in downs:
        ref, s, k, zz = source(name)
        put(ref.at[:GROUP], zz, k)
        if 0 < s < 4:
            put(ref.at[pl.ds(GROUP + 8, GROUP)], zz, 1 - k)
    for i, name in enumerate(biases):
        copy(source(name)[0].at[pl.ds(GROUP, 8)], part.at[i])
    where = {
        "f": (x, c), "g": (x, o),
        "x1f": (xs(side(c)), c), "x1g": (xs(side(c)), o),
        "ex1f": (xs(side(o)), o), "ex1g": (xs(side(o)), c),
        "x2f": (xs(2), c), "x2g": (xs(2), o), "ex2f": (xs(2), o),
    }
    for name in ups:
        xx, k = where[name]
        at = 0
        for s in range(5):
            zz = lax.rem(z - s * side(k) + Z, Z)
            for cc in (k, 1 - k)[: 2 if 0 < s < 4 else 1]:
                row = pl.multiple_of(((xx * 2 + lax.rem(zz, 2)) * 2 + cc) * 64, 64)
                copy(pieces[name].at[at : at + 64], up_out.at[lax.div(zz, 2), pl.ds(row, 64)])
                at += 64
    for cp in copies:
        cp.wait()
    for i, name in enumerate(biases):
        v = part[i].astype(F32)
        row = pl.ds(lax.div(source(name)[3], 2), 1)
        for k in range(2):
            b = v[k : k + 1] + v[2 + k : 3 + k] + v[4 + k : 5 + k]
            bias_out[0][row, k * COLS : (k + 1) * COLS] = b


def place(ups, downs, biases, values, old=()):
    n = len(ups) + len(downs) + len(biases)
    more = (jax.ShapeDtypeStruct((ZH, GROUP), F32),) if biases else ()
    return pl.pallas_call(
        functools.partial(place_kernel, ups, downs, biases, len(old)),
        out_shape=(
            jax.ShapeDtypeStruct((ZH, D, GROUP), BF),
            jax.ShapeDtypeStruct((4, HID, COLS), BF),
            *more,
        ),
        in_specs=[ANY] * (n + len(old)),
        out_specs=(ANY, ANY) + (VMEM,) * len(more),
        scratch_shapes=[pltpu.VMEM((9, 8, COLS), BF), pltpu.SemaphoreType.DMA],
        input_output_aliases={n + i: i for i in range(len(old))},
        compiler_params=pltpu.CompilerParams(vmem_limit_bytes=2 * 2**20),
        cost_estimate=pl.CostEstimate(flops=10**6, bytes_accessed=2**23, transcendentals=0),
    )(*[values[k] for k in ups + downs + biases], *old)


def split_kernel(b_ref, o_ref):
    b = jnp.concatenate([b_ref[:, :COLS], b_ref[:, COLS:]], axis=0)
    hi = b.astype(BF)
    rest = b - hi.astype(F32)
    mid = rest.astype(BF)
    low = (rest - mid.astype(F32)).astype(BF)
    o_ref[...] = jnp.concatenate([hi, mid, low, jnp.zeros_like(low)], axis=0)


def split_bias(b):
    return pl.pallas_call(
        split_kernel,
        out_shape=jax.ShapeDtypeStruct((8, COLS), BF),
        in_specs=[VMEM],
        out_specs=VMEM,
        compiler_params=pltpu.CompilerParams(vmem_limit_bytes=8 * 2**20),
        name="split_bias",
    )(b[None])


def mlp_kernel(n_tok, *refs):
    toks, (up, bias, down), outs, (t_ref, h_ref) = (
        refs[:n_tok], refs[n_tok : n_tok + 3], refs[n_tok + 3 : -2], refs[-2:],
    )
    at = 0
    for t in toks:
        t_ref[at : at + t.shape[0]] = t[...]
        at += t.shape[0]

    @pl.loop(0, at // 256)
    def _(i):
        rows = pl.ds(pl.multiple_of(i * 256, 256), 256)
        for g in range(ZH):
            s = jnp.dot(t_ref[rows], up[g], preferred_element_type=F32) + bias[g : g + 1]
            h_ref[:, g * GROUP : (g + 1) * GROUP] = jax.nn.gelu(s).astype(BF)
        for j in range(4):
            o = jnp.dot(h_ref[...], down[j], preferred_element_type=F32)
            outs[j % 2][j // 2, rows] = o.astype(BF)


def mlp(toks, up, bias, down):
    rows = sum(t.shape[0] for t in toks)
    half = jax.ShapeDtypeStruct((2, rows, COLS), BF)
    return pl.pallas_call(
        functools.partial(mlp_kernel, len(toks)),
        out_shape=(half, half),
        in_specs=[VMEM] * (len(toks) + 3),
        out_specs=(VMEM, VMEM),
        scratch_shapes=[pltpu.VMEM((rows, D), BF), pltpu.VMEM((256, HID), BF)],
        compiler_params=pltpu.CompilerParams(vmem_limit_bytes=20 * 2**20),
        name="mlp",
        cost_estimate=pl.CostEstimate(
            flops=10**8, bytes_accessed=2**23, transcendentals=rows * HID
        ),
    )(*toks, up, bias, down)


def add_kernel(h, p_ref, r_ref, o_ref):
    o_ref[...] = (p_ref[h].astype(F32) + r_ref[h].astype(F32)).astype(BF)


def add_in(p, r, h):
    return pl.pallas_call(
        functools.partial(add_kernel, h),
        out_shape=jax.ShapeDtypeStruct(p.shape[1:], BF),
        in_specs=[VMEM] * 2,
        out_specs=VMEM,
        compiler_params=pltpu.CompilerParams(vmem_limit_bytes=8 * 2**20),
        name="add_in",
        cost_estimate=pl.CostEstimate(flops=10**6, bytes_accessed=2**20, transcendentals=0),
    )(p, r)


def sum_kernel(h, p0, p1, sum0, one0, one1, sum1, bias_ref, *outs):
    x = lax.axis_index("x")
    for j, (p, full, part) in enumerate(((p0, sum0, one0), (p1, sum1, one1))):
        cols = pl.ds(pl.multiple_of(x * NX + (2 * h + j) * COLS, COLS), COLS)
        v = p[h].astype(F32) + full[...].astype(F32) + part[h].astype(F32)
        v = (v + bias_ref[:, cols]).astype(BF)
        for i, o in enumerate(outs):
            o[j] = v[i * TOK : (i + 1) * TOK]


def sum_up(h, *values):
    return pl.pallas_call(
        functools.partial(sum_kernel, h),
        out_shape=(jax.ShapeDtypeStruct((2, TOK, COLS), BF),) * 4,
        in_specs=[VMEM] * 7,
        out_specs=(VMEM,) * 4,
        compiler_params=pltpu.CompilerParams(vmem_limit_bytes=8 * 2**20),
        name="sum_up",
        cost_estimate=pl.CostEstimate(flops=10**6, bytes_accessed=2**20, transcendentals=0),
    )(*values)


def out_kernel(*refs):
    pieces, o_ref, sem = refs[:-2], refs[-2], refs[-1]
    x = lax.axis_index("x")
    copies = []
    for i, ref in enumerate(pieces):
        h, r = divmod(i, 4)
        xx = lax.rem(x + (0, X - 1, 1, 2)[r], X)
        for j in range(2):
            col = pl.multiple_of(xx * NX + h * 512 + j * 256, 256)
            cp = pltpu.make_async_copy(ref.at[j], o_ref.at[:, pl.ds(col, COLS)], sem)
            cp.start()
            copies.append(cp)
    for cp in copies:
        cp.wait()


def put_out(pieces):
    return pl.pallas_call(
        out_kernel,
        out_shape=jax.ShapeDtypeStruct((TOK, X * NX), BF),
        in_specs=[VMEM] * len(pieces),
        out_specs=ANY,
        scratch_shapes=[pltpu.SemaphoreType.DMA],
        compiler_params=pltpu.CompilerParams(vmem_limit_bytes=8 * 2**20),
        name="put_out",
    )(*pieces)


def step(patch_tokens, norm_gain, norm_bias, up_weight, up_bias, down_weight, down_bias):
    own = normalize(patch_tokens, norm_gain, norm_bias)
    left, right = on_x(own, 1), on_x(own, -1)
    below = [on_y(own, 1)]
    above = [on_y(own, -1)]
    across = [on_x(left[:64], 1), on_x(right[64:], -1)]
    rest = jnp.concatenate([left, right, *across], axis=0)
    below.append(on_y(rest, 1))
    above.append(on_y(rest, -1))
    far = [
        on_y(below[0][:64], 1), on_y(above[0][64:], -1),
        on_y(below[1][:192], 1), on_y(above[1][192:], -1),
    ]

    u = [jnp.concatenate([up_weight, on_c(up_weight)], axis=0)]
    for _ in range(3):
        u.append(on_z(u[-1], -1))
    u4 = on_z(u[3][:64], -1)
    f = jnp.concatenate([up_weight, u[1], u[2], u[3], u4], axis=0)
    g = on_c(f)
    x1f, x1g = on_xc(f), on_xc(g)
    x2f = on_xc(x1f)
    pieces = dict(f=f, g=g, x1f=x1f, x1g=x1g, x2f=x2f, ex1f=on_c(x1f))
    pieces |= dict(ex1g=on_c(x1g), ex2f=on_c(x2f))

    d_other = on_c(down_weight)
    w = [jnp.concatenate([down_weight, split_bias(up_bias), d_other], axis=0)]
    for _ in range(3):
        w.append(on_z(w[-1], 1))
    w.append(on_z(w[3][: GROUP + 8], 1))
    pieces |= dict(w0=w[0], e0=d_other)
    for k, a in enumerate(w[1:], 1):
        pieces |= {f"w{k}": a, f"e{k}": on_c(a)}

    early = place(UP_EARLY, DOWN_EARLY, (), pieces)
    up, down, bias = place(UP_LATE, DOWN_LATE, BIASES, pieces, early)
    far0, far1 = mlp(far, up, bias, down)
    from_below, from_above = on_y(far0, 1), on_y(far1, -1)
    above0, above1 = mlp(above, up, bias, down)
    one1 = on_y(above1, 1)
    below0, below1 = mlp(below, up, bias, down)
    one0 = on_y(below0, -1)
    own0, own1 = mlp([own, rest], up, bias, down)
    placed = []
    for h in range(2):
        sum0 = on_y(add_in(above0, from_below, h), 1)
        sum1 = on_y(add_in(below1, from_above, h), -1)
        values = (own0, own1, sum0, one0, one1, sum1, down_bias[None])
        mine, to_left, to_right, to_far = sum_up(h, *values)
        opposite = on_x(to_far, 2)
        placed += [mine, on_x(to_right, 1), on_x(to_left, -1), opposite]
    return put_out(placed)


def solution(mesh):
    grid = Mesh(mesh.devices.reshape(X, 2, 2, Y, ZH), ("x", "zl", "c", "y", "zh"))
    img, tp = ("x", "zl", "c"), ("y", "zh")
    return jax.shard_map(
        step,
        mesh=grid,
        in_specs=(P((*img, *tp), None), P(), P(), P(img, tp), P(tp), P(tp, img), P()),
        out_specs=P((*img, *tp), None),
        check_vma=False,
    )
```

```python
import functools

import jax
import jax.numpy as jnp
from jax import lax
from jax.experimental import pallas as pl
from jax.experimental.pallas import tpu as pltpu
from jax.sharding import Mesh
from jax.sharding import PartitionSpec as P


BF = jnp.bfloat16
F32 = jnp.float32
D, TOK = 1024, 128
X, Y, Z, ZH = 4, 4, 8, 4
GROUP = 512
COLS = 256
HID = ZH * GROUP
NX = 4 * COLS
ANY = pl.BlockSpec(memory_space=pl.ANY)
VMEM = pl.BlockSpec(memory_space=pltpu.VMEM)


def ring(n, d):
    return [(i, (i + d) % n) for i in range(n)]


def both_ways(n):
    return [(2 * i + c, 2 * ((i + (1 - 2 * c)) % n) + c) for i in range(n) for c in (0, 1)]


def on_x(a, d):
    return lax.ppermute(a, "x", ring(X, d))


def on_y(a, d):
    return lax.ppermute(a, "y", ring(Y, d))


def on_z(a):
    def at(i):
        return (i // 2 % 2 * 2 + i % 2) * ZH + i // 4

    return lax.ppermute(a, ("zl", "c", "zh"), [(at(i), at(j)) for i, j in both_ways(Z)])


def over_z(a):
    return lax.all_to_all(a, ("zl", "zh"), split_axis=0, concat_axis=0, tiled=True)


def on_xc(a):
    return lax.ppermute(a, ("x", "c"), both_ways(X))


def on_c(a):
    return lax.ppermute(a, "c", [(0, 1), (1, 0)])


def norm_kernel(x_ref, g_ref, b_ref, o_ref):
    @pl.loop(0, 4)
    def _(i):
        rows = pl.ds(pl.multiple_of(i * 32, 32), 32)
        v = x_ref[rows].astype(F32)
        center = jnp.mean(v, axis=1, keepdims=True)
        w = v - center
        spread = jnp.mean(w * w, axis=1, keepdims=True)
        o_ref[rows] = (w * lax.rsqrt(spread + 1e-05) * g_ref[...] + b_ref[...]).astype(BF)


def normalize(rows, gain, bias):
    return pl.pallas_call(
        norm_kernel,
        out_shape=jax.ShapeDtypeStruct(rows.shape, BF),
        in_specs=[VMEM] * 3,
        out_specs=VMEM,
        compiler_params=pltpu.CompilerParams(vmem_limit_bytes=8 * 2**20),
        name="norm",
        cost_estimate=pl.CostEstimate(flops=10**6, bytes_accessed=2**19, transcendentals=128),
    )(rows, gain[None], bias[None])


def side(c):
    return 2 * c - 1


UP_EARLY, UP_LATE = ("f", "g", "x1f", "x1g", "ex1f"), ("ex1g", "x2f", "ex2f")
DOWN_EARLY, DOWN_LATE = ("w0", "e0", "w1", "w2", "e1", "e2", "w3"), ("e3", "w4", "e4")
BIASES = ("w0", "w1", "w2", "w3", "w4", "e1", "e2", "e3", "e4")


def place_kernel(ups, downs, biases, n_old, *refs):
    n = len(ups) + len(downs) + len(biases)
    pieces = dict(zip(ups + downs + biases, refs))
    up_out, down_out, *bias_out, part, sem = refs[n + n_old :]
    x, c = lax.axis_index("x"), lax.axis_index("c")
    z = lax.axis_index("zh") * 2 + lax.axis_index("zl")
    o = 1 - c
    copies = []

    def copy(src, dst):
        cp = pltpu.make_async_copy(src, dst, sem)
        cp.start()
        copies.append(cp)

    def xs(d):
        return lax.rem(x + d + X, X)

    def put(src, zz, cc):
        row = pl.multiple_of(lax.div(zz, 2) * GROUP, GROUP)
        copy(src, down_out.at[lax.rem(zz, 2) * 2 + cc, pl.ds(row, GROUP)])

    def source(name):
        s, k = int(name[1]), c if name[0] == "w" else o
        return pieces[name], s, k, lax.rem(z + s * side(k) + Z, Z)

    for name in downs:
        ref, s, k, zz = source(name)
        put(ref.at[:GROUP], zz, k)
        if 0 < s < 4:
            put(ref.at[pl.ds(GROUP + 8, GROUP)], zz, 1 - k)
    for i, name in enumerate(biases):
        copy(source(name)[0].at[pl.ds(GROUP, 8)], part.at[i])
    where = {
        "f": (x, c), "g": (x, o),
        "x1f": (xs(side(c)), c), "x1g": (xs(side(c)), o),
        "ex1f": (xs(side(o)), o), "ex1g": (xs(side(o)), c),
        "x2f": (xs(2), c), "x2g": (xs(2), o), "ex2f": (xs(2), o),
    }
    for name in ups:
        xx, k = where[name]
        for zl in range(2):
            row = pl.multiple_of(((xx * 2 + zl) * 2 + k) * 64, 64)
            copy(pieces[name].at[zl * ZH : (zl + 1) * ZH], up_out.at[:, pl.ds(row, 64)])
    for cp in copies:
        cp.wait()
    for i, name in enumerate(biases):
        v = part[i].astype(F32)
        row = pl.ds(lax.div(source(name)[3], 2), 1)
        for k in range(2):
            b = v[k : k + 1] + v[2 + k : 3 + k] + v[4 + k : 5 + k]
            bias_out[0][row, k * COLS : (k + 1) * COLS] = b


def place(ups, downs, biases, values, old=()):
    n = len(ups) + len(downs) + len(biases)
    more = (jax.ShapeDtypeStruct((ZH, GROUP), F32),) if biases else ()
    return pl.pallas_call(
        functools.partial(place_kernel, ups, downs, biases, len(old)),
        out_shape=(
            jax.ShapeDtypeStruct((ZH, D, GROUP), BF),
            jax.ShapeDtypeStruct((4, HID, COLS), BF),
            *more,
        ),
        in_specs=[ANY] * (n + len(old)),
        out_specs=(ANY, ANY) + (VMEM,) * len(more),
        scratch_shapes=[pltpu.VMEM((9, 8, COLS), BF), pltpu.SemaphoreType.DMA],
        input_output_aliases={n + i: i for i in range(len(old))},
        compiler_params=pltpu.CompilerParams(vmem_limit_bytes=2 * 2**20),
        cost_estimate=pl.CostEstimate(flops=10**6, bytes_accessed=2**23, transcendentals=0),
    )(*[values[k] for k in ups + downs + biases], *old)


def split_kernel(b_ref, o_ref):
    b = jnp.concatenate([b_ref[:, :COLS], b_ref[:, COLS:]], axis=0)
    hi = b.astype(BF)
    rest = b - hi.astype(F32)
    mid = rest.astype(BF)
    low = (rest - mid.astype(F32)).astype(BF)
    o_ref[...] = jnp.concatenate([hi, mid, low, jnp.zeros_like(low)], axis=0)


def split_bias(b):
    return pl.pallas_call(
        split_kernel,
        out_shape=jax.ShapeDtypeStruct((8, COLS), BF),
        in_specs=[VMEM],
        out_specs=VMEM,
        compiler_params=pltpu.CompilerParams(vmem_limit_bytes=8 * 2**20),
        name="split_bias",
    )(b[None])


def mlp_kernel(plan, *refs):
    toks, (up, bias, down), outs, (t_ref, h_ref) = (
        refs[:-7], refs[-7:-4], refs[-4:-2], refs[-2:],
    )
    for t, parts in zip(toks, plan):
        for src, dst, n in parts:
            t_ref[dst : dst + n] = t[src : src + n]

    @pl.loop(0, 2)
    def _(i):
        rows = pl.ds(pl.multiple_of(i * 256, 256), 256)
        for g in range(ZH):
            s = jnp.dot(t_ref[rows], up[g], preferred_element_type=F32) + bias[g : g + 1]
            h_ref[:, g * GROUP : (g + 1) * GROUP] = jax.nn.gelu(s).astype(BF)
        for j in range(4):
            o = jnp.dot(h_ref[...], down[j], preferred_element_type=F32)
            outs[j % 2][j // 2, rows] = o.astype(BF)


def small_mlp_kernel(*refs):
    toks, (up, bias, down), outs, (t_ref, h_ref) = (
        refs[:-7], refs[-7:-4], refs[-4:-2], refs[-2:],
    )
    t_ref[0:128] = toks[0][...]
    t_ref[128:512] = toks[1][...]

    @pl.loop(0, 2)
    def _(i):
        rows = pl.ds(pl.multiple_of(i * 256, 256), 256)

        @pl.loop(0, ZH)
        def _(g):
            s = jnp.dot(t_ref[rows], up[g], preferred_element_type=F32) + bias[pl.ds(g, 1)]
            h_ref[:, pl.ds(pl.multiple_of(g * GROUP, GROUP), GROUP)] = jax.nn.gelu(s).astype(BF)

        @pl.loop(0, 2)
        def _(h):
            for j in range(2):
                o = jnp.dot(h_ref[...], down[2 * h + j], preferred_element_type=F32)
                outs[j][h, rows] = o.astype(BF)


def mlp(toks, plan, up, bias, down, small=False):
    rows = 512
    half = jax.ShapeDtypeStruct((2, rows, COLS), BF)
    return pl.pallas_call(
        small_mlp_kernel if small else functools.partial(mlp_kernel, plan),
        out_shape=(half, half),
        in_specs=[VMEM] * (len(toks) + 3),
        out_specs=(VMEM, VMEM),
        scratch_shapes=[pltpu.VMEM((rows, D), BF), pltpu.VMEM((256, HID), BF)],
        compiler_params=pltpu.CompilerParams(vmem_limit_bytes=20 * 2**20),
        name="mlp",
        cost_estimate=pl.CostEstimate(
            flops=10**8, bytes_accessed=2**23, transcendentals=rows * HID
        ),
    )(*toks, up, bias, down)


def add_kernel(h, p_ref, r_ref, o_ref):
    @pl.loop(0, 4)
    def _(i):
        rows = pl.ds(pl.multiple_of(i * TOK, TOK), TOK)
        o_ref[rows] = (p_ref[h, rows].astype(F32) + r_ref[h, rows].astype(F32)).astype(BF)


def add_in(p, r, h):
    return pl.pallas_call(
        functools.partial(add_kernel, h),
        out_shape=jax.ShapeDtypeStruct(p.shape[1:], BF),
        in_specs=[VMEM] * 2,
        out_specs=VMEM,
        compiler_params=pltpu.CompilerParams(vmem_limit_bytes=8 * 2**20),
        name="add_in",
        cost_estimate=pl.CostEstimate(flops=10**6, bytes_accessed=2**20, transcendentals=0),
    )(p, r)


def sum_kernel(h, p0, p1, sum0, one0, one1, sum1, bias_ref, *outs):
    x = lax.axis_index("x")

    @pl.loop(0, 4)
    def _(r):
        to = pl.ds(pl.multiple_of(r * 32, 32), 32)
        for i, o in enumerate(outs):
            rows = pl.ds(pl.multiple_of(i * TOK + r * 32, 32), 32)
            for j, (p, full, part) in enumerate(((p0, sum0, one0), (p1, sum1, one1))):
                cols = pl.ds(pl.multiple_of(x * NX + (2 * h + j) * COLS, COLS), COLS)
                v = p[h, rows].astype(F32) + full[rows].astype(F32) + part[h, rows].astype(F32)
                o[j, to] = (v + bias_ref[:, cols]).astype(BF)


def sum_up(h, *values):
    return pl.pallas_call(
        functools.partial(sum_kernel, h),
        out_shape=(jax.ShapeDtypeStruct((2, TOK, COLS), BF),) * 4,
        in_specs=[VMEM] * 7,
        out_specs=(VMEM,) * 4,
        compiler_params=pltpu.CompilerParams(vmem_limit_bytes=8 * 2**20),
        name="sum_up",
        cost_estimate=pl.CostEstimate(flops=10**6, bytes_accessed=2**20, transcendentals=0),
    )(*values)


def out_kernel(*refs):
    pieces, o_ref, sem = refs[:-2], refs[-2], refs[-1]
    x = lax.axis_index("x")
    copies = []
    for i, ref in enumerate(pieces):
        h, r = divmod(i, 4)
        xx = lax.rem(x + (0, X - 1, 1, 2)[r], X)
        for j in range(2):
            col = pl.multiple_of(xx * NX + h * 512 + j * 256, 256)
            cp = pltpu.make_async_copy(ref.at[j], o_ref.at[:, pl.ds(col, COLS)], sem)
            cp.start()
            copies.append(cp)
    for cp in copies:
        cp.wait()


def put_out(pieces):
    return pl.pallas_call(
        out_kernel,
        out_shape=jax.ShapeDtypeStruct((TOK, X * NX), BF),
        in_specs=[VMEM] * len(pieces),
        out_specs=ANY,
        scratch_shapes=[pltpu.SemaphoreType.DMA],
        compiler_params=pltpu.CompilerParams(vmem_limit_bytes=8 * 2**20),
        name="put_out",
    )(*pieces)


def step(patch_tokens, norm_gain, norm_bias, up_weight, up_bias, down_weight, down_bias):
    own = normalize(patch_tokens, norm_gain, norm_bias)
    left, right = on_x(own, 1), on_x(own, -1)
    below = [on_y(own, 1)]
    above = [on_y(own, -1)]
    rest = jnp.concatenate([left, right, on_x(own, 2)], axis=0)
    below.append(on_y(rest, 1))
    above.append(on_y(rest, -1))
    half0 = jnp.concatenate([below[0][:64], below[1][:192]], axis=0)
    half1 = jnp.concatenate([above[0][64:], above[1][192:]], axis=0)
    far = [on_y(half0, 1), on_y(half1, -1)]

    copies = jnp.broadcast_to(up_weight, (Z, *up_weight.shape))
    f = over_z(copies)
    g = on_c(f)
    x1f, x1g = on_xc(f), on_xc(g)
    x2f = on_xc(x1f)
    pieces = dict(f=f, g=g, x1f=x1f, x1g=x1g, x2f=x2f, ex1f=on_c(x1f))
    pieces |= dict(ex1g=on_c(x1g), ex2f=on_c(x2f))

    d_other = on_c(down_weight)
    w = [jnp.concatenate([down_weight, split_bias(up_bias), d_other], axis=0)]
    for _ in range(3):
        w.append(on_z(w[-1]))
    w.append(on_z(w[3][: GROUP + 8]))
    pieces |= dict(w0=w[0], e0=d_other)
    for k, a in enumerate(w[1:], 1):
        pieces |= {f"w{k}": a, f"e{k}": on_c(a)}

    early = place(UP_EARLY, DOWN_EARLY, (), pieces)
    up, down, bias = place(UP_LATE, DOWN_LATE, BIASES, pieces, early)
    halves = (((0, 0, 64), (64, 128, 192)), ((0, 64, 64), (64, 320, 192)))
    wholes = (((0, 0, 128),), ((0, 128, 384),))
    far0, far1 = mlp(far, halves, up, bias, down)
    from_below, from_above = on_y(far0, 1), on_y(far1, -1)
    above0, above1 = mlp(above, wholes, up, bias, down)
    one1 = on_y(above1, 1)
    below0, below1 = mlp(below, wholes, up, bias, down)
    one0 = on_y(below0, -1)
    own0, own1 = mlp([own, rest], wholes, up, bias, down, True)
    placed = []
    for h in range(2):
        sum0 = on_y(add_in(above0, from_below, h), 1)
        sum1 = on_y(add_in(below1, from_above, h), -1)
        values = (own0, own1, sum0, one0, one1, sum1, down_bias[None])
        mine, to_left, to_right, to_far = sum_up(h, *values)
        opposite = on_x(to_far, 2)
        placed += [mine, on_x(to_right, 1), on_x(to_left, -1), opposite]
    return put_out(placed)


def solution(mesh):
    grid = Mesh(mesh.devices.reshape(X, 2, 2, Y, ZH), ("x", "zl", "c", "y", "zh"))
    img, tp = ("x", "zl", "c"), ("y", "zh")
    return jax.shard_map(
        step,
        mesh=grid,
        in_specs=(P((*img, *tp), None), P(), P(), P(img, tp), P(tp), P(tp, img), P()),
        out_specs=P((*img, *tp), None),
        check_vma=False,
    )
```

```python
import functools

import jax
import jax.numpy as jnp
from jax import lax
from jax.experimental import pallas as pl
from jax.experimental.pallas import tpu as pltpu
from jax.sharding import Mesh
from jax.sharding import PartitionSpec as P


BF = jnp.bfloat16
F32 = jnp.float32
D, TOK = 1024, 128
X, Y, Z, ZH = 4, 4, 8, 4
GROUP = 512
COLS = 256
HID = ZH * GROUP
NX = 4 * COLS
ANY = pl.BlockSpec(memory_space=pl.ANY)
VMEM = pl.BlockSpec(memory_space=pltpu.VMEM)


def ring(n, d):
    return [(i, (i + d) % n) for i in range(n)]


def both_ways(n):
    return [(2 * i + c, 2 * ((i + (1 - 2 * c)) % n) + c) for i in range(n) for c in (0, 1)]


def on_x(a, d):
    return lax.ppermute(a, "x", ring(X, d))


def on_y(a, d):
    return lax.ppermute(a, "y", ring(Y, d))


def on_z(a):
    def at(i):
        return (i // 2 % 2 * 2 + i % 2) * ZH + i // 4

    return lax.ppermute(a, ("zl", "c", "zh"), [(at(i), at(j)) for i, j in both_ways(Z)])


def over_z(a):
    return lax.all_to_all(a, ("zl", "zh"), split_axis=0, concat_axis=0, tiled=True)


def on_xc(a):
    return lax.ppermute(a, ("x", "c"), both_ways(X))


def on_c(a):
    return lax.ppermute(a, "c", [(0, 1), (1, 0)])


def norm_kernel(x_ref, g_ref, b_ref, o_ref):
    @pl.loop(0, 4)
    def _(i):
        rows = pl.ds(pl.multiple_of(i * 32, 32), 32)
        v = x_ref[rows].astype(F32)
        center = jnp.mean(v, axis=1, keepdims=True)
        w = v - center
        spread = jnp.mean(w * w, axis=1, keepdims=True)
        o_ref[rows] = (w * lax.rsqrt(spread + 1e-05) * g_ref[...] + b_ref[...]).astype(BF)


def normalize(rows, gain, bias):
    return pl.pallas_call(
        norm_kernel,
        out_shape=jax.ShapeDtypeStruct(rows.shape, BF),
        in_specs=[VMEM] * 3,
        out_specs=VMEM,
        compiler_params=pltpu.CompilerParams(vmem_limit_bytes=8 * 2**20),
        name="norm",
        cost_estimate=pl.CostEstimate(flops=10**6, bytes_accessed=2**19, transcendentals=128),
    )(rows, gain[None], bias[None])


def copies_kernel(w_ref, o_ref):
    @pl.loop(0, Z)
    def _(i):
        o_ref[i] = w_ref[...]


def copies_of(w):
    return pl.pallas_call(
        copies_kernel,
        out_shape=jax.ShapeDtypeStruct((Z, *w.shape), BF),
        in_specs=[VMEM],
        out_specs=VMEM,
        compiler_params=pltpu.CompilerParams(vmem_limit_bytes=2 * 2**20),
        name="copies",
        cost_estimate=pl.CostEstimate(flops=10**5, bytes_accessed=2**19, transcendentals=0),
    )(w)


def side(c):
    return 2 * c - 1


UP_EARLY, UP_LATE = ("f", "g", "x1f", "x1g", "ex1f"), ("ex1g", "x2f", "ex2f")
DOWN_EARLY, DOWN_LATE = ("w0", "e0", "w1", "w2", "e1", "e2", "w3"), ("e3", "w4", "e4")
BIASES = ("w0", "w1", "w2", "w3", "w4", "e1", "e2", "e3", "e4")


def place_kernel(ups, downs, biases, n_old, *refs):
    n = len(ups) + len(downs) + len(biases)
    pieces = dict(zip(ups + downs + biases, refs))
    up_out, down_out, *bias_out, part, sem = refs[n + n_old :]
    x, c = lax.axis_index("x"), lax.axis_index("c")
    z = lax.axis_index("zh") * 2 + lax.axis_index("zl")
    o = 1 - c
    copies = []

    def copy(src, dst):
        cp = pltpu.make_async_copy(src, dst, sem)
        cp.start()
        copies.append(cp)

    def xs(d):
        return lax.rem(x + d + X, X)

    def put(src, zz, cc):
        row = pl.multiple_of(lax.div(zz, 2) * GROUP, GROUP)
        copy(src, down_out.at[lax.rem(zz, 2) * 2 + cc, pl.ds(row, GROUP)])

    def source(name):
        s, k = int(name[1]), c if name[0] == "w" else o
        return pieces[name], s, k, lax.rem(z + s * side(k) + Z, Z)

    for name in downs:
        ref, s, k, zz = source(name)
        put(ref.at[:GROUP], zz, k)
        if 0 < s < 4:
            put(ref.at[pl.ds(GROUP + 8, GROUP)], zz, 1 - k)
    for i, name in enumerate(biases):
        copy(source(name)[0].at[pl.ds(GROUP, 8)], part.at[i])
    where = {
        "f": (x, c), "g": (x, o),
        "x1f": (xs(side(c)), c), "x1g": (xs(side(c)), o),
        "ex1f": (xs(side(o)), o), "ex1g": (xs(side(o)), c),
        "x2f": (xs(2), c), "x2g": (xs(2), o), "ex2f": (xs(2), o),
    }
    for name in ups:
        xx, k = where[name]
        for zl in range(2):
            row = pl.multiple_of(((xx * 2 + zl) * 2 + k) * 64, 64)
            copy(pieces[name].at[zl * ZH : (zl + 1) * ZH], up_out.at[:, pl.ds(row, 64)])
    for cp in copies:
        cp.wait()
    for i, name in enumerate(biases):
        v = part[i].astype(F32)
        row = pl.ds(lax.div(source(name)[3], 2), 1)
        for k in range(2):
            b = v[k : k + 1] + v[2 + k : 3 + k] + v[4 + k : 5 + k]
            bias_out[0][row, k * COLS : (k + 1) * COLS] = b


def place(ups, downs, biases, values, old=()):
    n = len(ups) + len(downs) + len(biases)
    more = (jax.ShapeDtypeStruct((ZH, GROUP), F32),) if biases else ()
    return pl.pallas_call(
        functools.partial(place_kernel, ups, downs, biases, len(old)),
        out_shape=(
            jax.ShapeDtypeStruct((ZH, D, GROUP), BF),
            jax.ShapeDtypeStruct((4, HID, COLS), BF),
            *more,
        ),
        in_specs=[ANY] * (n + len(old)),
        out_specs=(ANY, ANY) + (VMEM,) * len(more),
        scratch_shapes=[pltpu.VMEM((9, 8, COLS), BF), pltpu.SemaphoreType.DMA],
        input_output_aliases={n + i: i for i in range(len(old))},
        compiler_params=pltpu.CompilerParams(vmem_limit_bytes=2 * 2**20),
        cost_estimate=pl.CostEstimate(flops=10**6, bytes_accessed=2**23, transcendentals=0),
    )(*[values[k] for k in ups + downs + biases], *old)


def split_kernel(b_ref, o_ref):
    b = jnp.concatenate([b_ref[:, :COLS], b_ref[:, COLS:]], axis=0)
    hi = b.astype(BF)
    rest = b - hi.astype(F32)
    mid = rest.astype(BF)
    low = (rest - mid.astype(F32)).astype(BF)
    o_ref[...] = jnp.concatenate([hi, mid, low, jnp.zeros_like(low)], axis=0)


def split_bias(b):
    return pl.pallas_call(
        split_kernel,
        out_shape=jax.ShapeDtypeStruct((8, COLS), BF),
        in_specs=[VMEM],
        out_specs=VMEM,
        compiler_params=pltpu.CompilerParams(vmem_limit_bytes=8 * 2**20),
        name="split_bias",
    )(b[None])


def fill(t_ref, toks, plan):
    for t, parts in zip(toks, plan):
        for src, dst, n in parts:
            t_ref[dst : dst + n] = t[src : src + n]


def mlp_kernel(plan, *refs):
    toks, (up, bias, down), outs, (t_ref, h_ref) = (
        refs[:-7], refs[-7:-4], refs[-4:-2], refs[-2:],
    )
    fill(t_ref, toks, plan)

    @pl.loop(0, 2)
    def _(i):
        rows = pl.ds(pl.multiple_of(i * 256, 256), 256)
        for g in range(ZH):
            s = jnp.dot(t_ref[rows], up[g], preferred_element_type=F32) + bias[g : g + 1]
            h_ref[:, g * GROUP : (g + 1) * GROUP] = jax.nn.gelu(s).astype(BF)
        for j in range(4):
            o = jnp.dot(h_ref[...], down[j], preferred_element_type=F32)
            outs[j % 2][j // 2, rows] = o.astype(BF)


def short_mlp_kernel(plan, *refs):
    toks, (up, bias, down), outs, (t_ref, h_ref) = (
        refs[:-7], refs[-7:-4], refs[-4:-2], refs[-2:],
    )
    fill(t_ref, toks, plan)

    @pl.loop(0, 2)
    def _(i):
        rows = pl.ds(pl.multiple_of(i * 256, 256), 256)

        @pl.loop(0, ZH)
        def _(g):
            s = jnp.dot(t_ref[rows], up[g], preferred_element_type=F32) + bias[pl.ds(g, 1)]
            h_ref[:, pl.ds(pl.multiple_of(g * GROUP, GROUP), GROUP)] = jax.nn.gelu(s).astype(BF)

        @pl.loop(0, 2)
        def _(h):
            for j in range(2):
                o = jnp.dot(h_ref[...], down[2 * h + j], preferred_element_type=F32)
                outs[j][h, rows] = o.astype(BF)


def mlp(toks, plan, up, bias, down, kernel=mlp_kernel):
    half = jax.ShapeDtypeStruct((2, 512, COLS), BF)
    return pl.pallas_call(
        functools.partial(kernel, plan),
        out_shape=(half, half),
        in_specs=[VMEM] * (len(toks) + 3),
        out_specs=(VMEM, VMEM),
        scratch_shapes=[pltpu.VMEM((512, D), BF), pltpu.VMEM((256, HID), BF)],
        compiler_params=pltpu.CompilerParams(vmem_limit_bytes=20 * 2**20),
        name="mlp",
        cost_estimate=pl.CostEstimate(
            flops=10**8, bytes_accessed=2**23, transcendentals=512 * HID
        ),
    )(*toks, up, bias, down)


def add_kernel(h, p_ref, r_ref, o_ref):
    @pl.loop(0, 4)
    def _(i):
        rows = pl.ds(pl.multiple_of(i * TOK, TOK), TOK)
        o_ref[rows] = (p_ref[h, rows].astype(F32) + r_ref[h, rows].astype(F32)).astype(BF)


def add_in(p, r, h):
    return pl.pallas_call(
        functools.partial(add_kernel, h),
        out_shape=jax.ShapeDtypeStruct(p.shape[1:], BF),
        in_specs=[VMEM] * 2,
        out_specs=VMEM,
        compiler_params=pltpu.CompilerParams(vmem_limit_bytes=8 * 2**20),
        name="add_in",
        cost_estimate=pl.CostEstimate(flops=10**6, bytes_accessed=2**20, transcendentals=0),
    )(p, r)


def sum_kernel(h, p0, p1, sum0, one0, one1, sum1, bias_ref, *outs):
    x = lax.axis_index("x")

    @pl.loop(0, 4)
    def _(r):
        to = pl.ds(pl.multiple_of(r * 32, 32), 32)
        for i, o in enumerate(outs):
            rows = pl.ds(pl.multiple_of(i * TOK + r * 32, 32), 32)
            for j, (p, full, part) in enumerate(((p0, sum0, one0), (p1, sum1, one1))):
                cols = pl.ds(pl.multiple_of(x * NX + (2 * h + j) * COLS, COLS), COLS)
                v = p[h, rows].astype(F32) + full[rows].astype(F32) + part[h, rows].astype(F32)
                o[j, to] = (v + bias_ref[:, cols]).astype(BF)


def sum_up(h, *values):
    return pl.pallas_call(
        functools.partial(sum_kernel, h),
        out_shape=(jax.ShapeDtypeStruct((2, TOK, COLS), BF),) * 4,
        in_specs=[VMEM] * 7,
        out_specs=(VMEM,) * 4,
        compiler_params=pltpu.CompilerParams(vmem_limit_bytes=8 * 2**20),
        name="sum_up",
        cost_estimate=pl.CostEstimate(flops=10**6, bytes_accessed=2**20, transcendentals=0),
    )(*values)


def out_kernel(*refs):
    pieces, o_ref, sem = refs[:-2], refs[-2], refs[-1]
    x = lax.axis_index("x")
    copies = []
    for i, ref in enumerate(pieces):
        h, r = divmod(i, 4)
        xx = lax.rem(x + (0, X - 1, 1, 2)[r], X)
        for j in range(2):
            col = pl.multiple_of(xx * NX + h * 512 + j * 256, 256)
            cp = pltpu.make_async_copy(ref.at[j], o_ref.at[:, pl.ds(col, COLS)], sem)
            cp.start()
            copies.append(cp)
    for cp in copies:
        cp.wait()


def put_out(pieces):
    return pl.pallas_call(
        out_kernel,
        out_shape=jax.ShapeDtypeStruct((TOK, X * NX), BF),
        in_specs=[VMEM] * len(pieces),
        out_specs=ANY,
        scratch_shapes=[pltpu.SemaphoreType.DMA],
        compiler_params=pltpu.CompilerParams(vmem_limit_bytes=8 * 2**20),
        name="put_out",
    )(*pieces)


def step(patch_tokens, norm_gain, norm_bias, up_weight, up_bias, down_weight, down_bias):
    own = normalize(patch_tokens, norm_gain, norm_bias)
    left, right = on_x(own, 1), on_x(own, -1)
    below = [on_y(own, 1)]
    above = [on_y(own, -1)]
    rest = jnp.concatenate([left, right, on_x(own, 2)], axis=0)
    below.append(on_y(rest, 1))
    above.append(on_y(rest, -1))
    half0 = jnp.concatenate([below[0][:64], below[1][:192]], axis=0)
    half1 = jnp.concatenate([above[0][64:], above[1][192:]], axis=0)
    far = [on_y(half0, 1), on_y(half1, -1)]

    f = over_z(copies_of(up_weight))
    g = on_c(f)
    x1f, x1g = on_xc(f), on_xc(g)
    x2f = on_xc(x1f)
    pieces = dict(f=f, g=g, x1f=x1f, x1g=x1g, x2f=x2f, ex1f=on_c(x1f))
    pieces |= dict(ex1g=on_c(x1g), ex2f=on_c(x2f))

    d_other = on_c(down_weight)
    w = [jnp.concatenate([down_weight, split_bias(up_bias), d_other], axis=0)]
    for _ in range(3):
        w.append(on_z(w[-1]))
    w.append(on_z(w[3][: GROUP + 8]))
    pieces |= dict(w0=w[0], e0=d_other)
    for k, a in enumerate(w[1:], 1):
        pieces |= {f"w{k}": a, f"e{k}": on_c(a)}

    early = place(UP_EARLY, DOWN_EARLY, (), pieces)
    up, down, bias = place(UP_LATE, DOWN_LATE, BIASES, pieces, early)
    halves = (((0, 0, 64), (64, 128, 192)), ((0, 64, 64), (64, 320, 192)))
    wholes = (((0, 0, 128),), ((0, 128, 384),))
    above0, above1 = mlp(above, wholes, up, bias, down)
    one1 = on_y(above1, 1)
    far0, far1 = mlp(far, halves, up, bias, down)
    from_below, from_above = on_y(far0, 1), on_y(far1, -1)
    below0, below1 = mlp(below, wholes, up, bias, down)
    one0 = on_y(below0, -1)
    own0, own1 = mlp([own, rest], wholes, up, bias, down, short_mlp_kernel)
    placed = []
    for h in range(2):
        sum0 = on_y(add_in(above0, from_below, h), 1)
        sum1 = on_y(add_in(below1, from_above, h), -1)
        values = (own0, own1, sum0, one0, one1, sum1, down_bias[None])
        mine, to_left, to_right, to_far = sum_up(h, *values)
        opposite = on_x(to_far, 2)
        placed += [mine, on_x(to_right, 1), on_x(to_left, -1), opposite]
    return put_out(placed)


def solution(mesh):
    grid = Mesh(mesh.devices.reshape(X, 2, 2, Y, ZH), ("x", "zl", "c", "y", "zh"))
    img, tp = ("x", "zl", "c"), ("y", "zh")
    return jax.shard_map(
        step,
        mesh=grid,
        in_specs=(P((*img, *tp), None), P(), P(), P(img, tp), P(tp), P(tp, img), P()),
        out_specs=P((*img, *tp), None),
        check_vma=False,
    )
```

```python
import functools

import jax
import jax.numpy as jnp
from jax import lax
from jax.experimental import pallas as pl
from jax.experimental.pallas import tpu as pltpu
from jax.sharding import Mesh
from jax.sharding import PartitionSpec as P


BF = jnp.bfloat16
F32 = jnp.float32
D, TOK = 1024, 128
X, Y, Z, ZH = 4, 4, 8, 4
GROUP = 512
COLS = 256
HID = ZH * GROUP
NX = 4 * COLS
ANY = pl.BlockSpec(memory_space=pl.ANY)
VMEM = pl.BlockSpec(memory_space=pltpu.VMEM)


def ring(n, d):
    return [(i, (i + d) % n) for i in range(n)]


def both_ways(n, d=1):
    return [(2 * i + c, 2 * ((i + d - 2 * d * c) % n) + c) for i in range(n) for c in (0, 1)]


def on_x(a, d):
    return lax.ppermute(a, "x", ring(X, d))


def on_y(a, d):
    return lax.ppermute(a, "y", ring(Y, d))


def on_z(a, d):
    def at(i):
        return (i // 2 % 2 * 2 + i % 2) * ZH + i // 4

    return lax.ppermute(a, ("zl", "c", "zh"), [(at(i), at(j)) for i, j in both_ways(Z, d)])


def over_z(a):
    return lax.all_to_all(a, ("zl", "zh"), split_axis=0, concat_axis=0, tiled=True)


def on_xc(a):
    return lax.ppermute(a, ("x", "c"), both_ways(X))


def on_c(a):
    return lax.ppermute(a, "c", [(0, 1), (1, 0)])


def norm_kernel(x_ref, g_ref, b_ref, o_ref):
    @pl.loop(0, 4)
    def _(i):
        rows = pl.ds(pl.multiple_of(i * 32, 32), 32)
        v = x_ref[rows].astype(F32)
        center = jnp.mean(v, axis=1, keepdims=True)
        w = v - center
        spread = jnp.mean(w * w, axis=1, keepdims=True)
        o_ref[rows] = (w * lax.rsqrt(spread + 1e-05) * g_ref[...] + b_ref[...]).astype(BF)


def normalize(rows, gain, bias):
    return pl.pallas_call(
        norm_kernel,
        out_shape=jax.ShapeDtypeStruct(rows.shape, BF),
        in_specs=[VMEM] * 3,
        out_specs=VMEM,
        compiler_params=pltpu.CompilerParams(vmem_limit_bytes=8 * 2**20),
        name="norm",
        cost_estimate=pl.CostEstimate(flops=10**6, bytes_accessed=2**19, transcendentals=128),
    )(rows, gain[None], bias[None])


def copies_kernel(w_ref, o_ref):
    @pl.loop(0, Z)
    def _(i):
        o_ref[i] = w_ref[...]


def copies_of(w):
    return pl.pallas_call(
        copies_kernel,
        out_shape=jax.ShapeDtypeStruct((Z, *w.shape), BF),
        in_specs=[VMEM],
        out_specs=VMEM,
        compiler_params=pltpu.CompilerParams(vmem_limit_bytes=2 * 2**20),
        name="copies",
        cost_estimate=pl.CostEstimate(flops=10**5, bytes_accessed=2**19, transcendentals=0),
    )(w)


def side(c):
    return 2 * c - 1


UP_EARLY, UP_LATE = ("f", "g", "x1f", "x1g", "ex1f"), ("ex1g", "x2f", "ex2f")
DOWN_EARLY, DOWN_LATE = ("w0", "e0", "w1", "w2", "e1", "e2", "w3"), ("e3", "w4", "e4")
BIASES = ("w0", "w1", "w2", "w3", "w4", "e1", "e2", "e3", "e4")


def place_kernel(ups, downs, biases, n_old, *refs):
    n = len(ups) + len(downs) + len(biases)
    pieces = dict(zip(ups + downs + biases, refs))
    up_out, down_out, *bias_out, part, sem = refs[n + n_old :]
    x, c = lax.axis_index("x"), lax.axis_index("c")
    z = lax.axis_index("zh") * 2 + lax.axis_index("zl")
    o = 1 - c
    copies = []

    def copy(src, dst):
        cp = pltpu.make_async_copy(src, dst, sem)
        cp.start()
        copies.append(cp)

    def xs(d):
        return lax.rem(x + d + X, X)

    def put(src, zz, cc):
        row = pl.multiple_of(lax.div(zz, 2) * GROUP, GROUP)
        copy(src, down_out.at[lax.rem(zz, 2) * 2 + cc, pl.ds(row, GROUP)])

    def source(name):
        s, k = int(name[1]), c if name[0] == "w" else o
        return pieces[name], s, k, lax.rem(z + s * side(k) + Z, Z)

    for name in downs:
        ref, s, k, zz = source(name)
        put(ref.at[:GROUP], zz, k)
        if 0 < s < 4:
            put(ref.at[pl.ds(GROUP + 8, GROUP)], zz, 1 - k)
    for i, name in enumerate(biases):
        copy(source(name)[0].at[pl.ds(GROUP, 8)], part.at[i])
    where = {
        "f": (x, c), "g": (x, o),
        "x1f": (xs(side(c)), c), "x1g": (xs(side(c)), o),
        "ex1f": (xs(side(o)), o), "ex1g": (xs(side(o)), c),
        "x2f": (xs(2), c), "x2g": (xs(2), o), "ex2f": (xs(2), o),
    }
    for name in ups:
        xx, k = where[name]
        for zl in range(2):
            row = pl.multiple_of(((xx * 2 + zl) * 2 + k) * 64, 64)
            copy(pieces[name].at[zl * ZH : (zl + 1) * ZH], up_out.at[:, pl.ds(row, 64)])
    for cp in copies:
        cp.wait()
    for i, name in enumerate(biases):
        v = part[i].astype(F32)
        row = pl.ds(lax.div(source(name)[3], 2), 1)
        for k in range(2):
            b = v[k : k + 1] + v[2 + k : 3 + k] + v[4 + k : 5 + k]
            bias_out[0][row, k * COLS : (k + 1) * COLS] = b


def place(ups, downs, biases, values, old=()):
    n = len(ups) + len(downs) + len(biases)
    more = (jax.ShapeDtypeStruct((ZH, GROUP), F32),) if biases else ()
    return pl.pallas_call(
        functools.partial(place_kernel, ups, downs, biases, len(old)),
        out_shape=(
            jax.ShapeDtypeStruct((ZH, D, GROUP), BF),
            jax.ShapeDtypeStruct((4, HID, COLS), BF),
            *more,
        ),
        in_specs=[ANY] * (n + len(old)),
        out_specs=(ANY, ANY) + (VMEM,) * len(more),
        scratch_shapes=[pltpu.VMEM((9, 8, COLS), BF), pltpu.SemaphoreType.DMA],
        input_output_aliases={n + i: i for i in range(len(old))},
        compiler_params=pltpu.CompilerParams(vmem_limit_bytes=2 * 2**20),
        cost_estimate=pl.CostEstimate(flops=10**6, bytes_accessed=2**23, transcendentals=0),
    )(*[values[k] for k in ups + downs + biases], *old)


def split_kernel(b_ref, o_ref):
    b = jnp.concatenate([b_ref[:, :COLS], b_ref[:, COLS:]], axis=0)
    hi = b.astype(BF)
    rest = b - hi.astype(F32)
    mid = rest.astype(BF)
    low = (rest - mid.astype(F32)).astype(BF)
    o_ref[...] = jnp.concatenate([hi, mid, low, jnp.zeros_like(low)], axis=0)


def split_bias(b):
    return pl.pallas_call(
        split_kernel,
        out_shape=jax.ShapeDtypeStruct((8, COLS), BF),
        in_specs=[VMEM],
        out_specs=VMEM,
        compiler_params=pltpu.CompilerParams(vmem_limit_bytes=8 * 2**20),
        name="split_bias",
    )(b[None])


def fill(t_ref, toks, plan):
    for t, parts in zip(toks, plan):
        for src, dst, n in parts:
            t_ref[dst : dst + n] = t[src : src + n]


def mlp_kernel(plan, *refs):
    toks, (up, bias, down), outs, (t_ref, h_ref) = (
        refs[:-7], refs[-7:-4], refs[-4:-2], refs[-2:],
    )
    fill(t_ref, toks, plan)

    @pl.loop(0, 2)
    def _(i):
        rows = pl.ds(pl.multiple_of(i * 256, 256), 256)
        for g in range(ZH):
            s = jnp.dot(t_ref[rows], up[g], preferred_element_type=F32) + bias[g : g + 1]
            h_ref[:, g * GROUP : (g + 1) * GROUP] = jax.nn.gelu(s).astype(BF)
        for j in range(4):
            o = jnp.dot(h_ref[...], down[j], preferred_element_type=F32)
            outs[j % 2][j // 2, rows] = o.astype(BF)


def short_mlp_kernel(plan, *refs):
    toks, (up, bias, down), outs, (t_ref, h_ref) = (
        refs[:-7], refs[-7:-4], refs[-4:-2], refs[-2:],
    )
    fill(t_ref, toks, plan)

    @pl.loop(0, 2)
    def _(i):
        rows = pl.ds(pl.multiple_of(i * 256, 256), 256)

        @pl.loop(0, ZH)
        def _(g):
            s = jnp.dot(t_ref[rows], up[g], preferred_element_type=F32) + bias[pl.ds(g, 1)]
            h_ref[:, pl.ds(pl.multiple_of(g * GROUP, GROUP), GROUP)] = jax.nn.gelu(s).astype(BF)

        @pl.loop(0, 2)
        def _(h):
            for j in range(2):
                o = jnp.dot(h_ref[...], down[2 * h + j], preferred_element_type=F32)
                outs[j][h, rows] = o.astype(BF)


def mlp(toks, plan, up, bias, down, kernel=mlp_kernel):
    half = jax.ShapeDtypeStruct((2, 512, COLS), BF)
    return pl.pallas_call(
        functools.partial(kernel, plan),
        out_shape=(half, half),
        in_specs=[VMEM] * (len(toks) + 3),
        out_specs=(VMEM, VMEM),
        scratch_shapes=[pltpu.VMEM((512, D), BF), pltpu.VMEM((256, HID), BF)],
        compiler_params=pltpu.CompilerParams(vmem_limit_bytes=12 * 2**20),
        name="mlp",
        cost_estimate=pl.CostEstimate(
            flops=10**8, bytes_accessed=2**23, transcendentals=512 * HID
        ),
    )(*toks, up, bias, down)


def add_kernel(h, p_ref, r_ref, o_ref):
    @pl.loop(0, 4)
    def _(i):
        rows = pl.ds(pl.multiple_of(i * TOK, TOK), TOK)
        o_ref[rows] = (p_ref[h, rows].astype(F32) + r_ref[h, rows].astype(F32)).astype(BF)


def add_in(p, r, h):
    return pl.pallas_call(
        functools.partial(add_kernel, h),
        out_shape=jax.ShapeDtypeStruct(p.shape[1:], BF),
        in_specs=[VMEM] * 2,
        out_specs=VMEM,
        compiler_params=pltpu.CompilerParams(vmem_limit_bytes=8 * 2**20),
        name="add_in",
        cost_estimate=pl.CostEstimate(flops=10**6, bytes_accessed=2**20, transcendentals=0),
    )(p, r)


def sum_kernel(h, p0, p1, sum0, one0, one1, sum1, bias_ref, *outs):
    x = lax.axis_index("x")

    @pl.loop(0, 4)
    def _(r):
        to = pl.ds(pl.multiple_of(r * 32, 32), 32)
        for i, o in enumerate(outs):
            rows = pl.ds(pl.multiple_of(i * TOK + r * 32, 32), 32)
            for j, (p, full, part) in enumerate(((p0, sum0, one0), (p1, sum1, one1))):
                cols = pl.ds(pl.multiple_of(x * NX + (2 * h + j) * COLS, COLS), COLS)
                v = p[h, rows].astype(F32) + full[rows].astype(F32) + part[h, rows].astype(F32)
                o[j, to] = (v + bias_ref[:, cols]).astype(BF)


def sum_up(h, *values):
    return pl.pallas_call(
        functools.partial(sum_kernel, h),
        out_shape=(jax.ShapeDtypeStruct((2, TOK, COLS), BF),) * 4,
        in_specs=[VMEM] * 7,
        out_specs=(VMEM,) * 4,
        compiler_params=pltpu.CompilerParams(vmem_limit_bytes=8 * 2**20),
        name="sum_up",
        cost_estimate=pl.CostEstimate(flops=10**6, bytes_accessed=2**20, transcendentals=0),
    )(*values)


def out_kernel(*refs):
    pieces, o_ref, sem = refs[:-2], refs[-2], refs[-1]
    x = lax.axis_index("x")
    copies = []
    for i, ref in enumerate(pieces):
        h, r = divmod(i, 4)
        xx = lax.rem(x + (0, X - 1, 1, 2)[r], X)
        for j in range(2):
            col = pl.multiple_of(xx * NX + h * 512 + j * 256, 256)
            cp = pltpu.make_async_copy(ref.at[j], o_ref.at[:, pl.ds(col, COLS)], sem)
            cp.start()
            copies.append(cp)
    for cp in copies:
        cp.wait()


def put_out(pieces):
    return pl.pallas_call(
        out_kernel,
        out_shape=jax.ShapeDtypeStruct((TOK, X * NX), BF),
        in_specs=[VMEM] * len(pieces),
        out_specs=ANY,
        scratch_shapes=[pltpu.SemaphoreType.DMA],
        compiler_params=pltpu.CompilerParams(vmem_limit_bytes=8 * 2**20),
        name="put_out",
    )(*pieces)


def step(patch_tokens, norm_gain, norm_bias, up_weight, up_bias, down_weight, down_bias):
    own = normalize(patch_tokens, norm_gain, norm_bias)
    left, right = on_x(own, 1), on_x(own, -1)
    below = [on_y(own, 1)]
    above = [on_y(own, -1)]
    rest = jnp.concatenate([left, right, on_x(own, 2)], axis=0)
    below.append(on_y(rest, 1))
    above.append(on_y(rest, -1))
    half0 = jnp.concatenate([below[0][:64], below[1][:192]], axis=0)
    half1 = jnp.concatenate([above[0][64:], above[1][192:]], axis=0)
    far = [on_y(half0, 1), on_y(half1, -1)]

    f = over_z(copies_of(up_weight))
    g = on_c(f)
    x1f, x1g = on_xc(f), on_xc(g)
    x2f = on_xc(x1f)
    pieces = dict(f=f, g=g, x1f=x1f, x1g=x1g, x2f=x2f, ex1f=on_c(x1f))
    pieces |= dict(ex1g=on_c(x1g), ex2f=on_c(x2f))

    d_other = on_c(down_weight)
    w = [jnp.concatenate([down_weight, split_bias(up_bias), d_other], axis=0)]
    w += [on_z(w[0], 1), on_z(w[0], 2)]
    w += [on_z(w[2], 1), on_z(w[2][: GROUP + 8], 2)]
    pieces |= dict(w0=w[0], e0=d_other)
    for k, a in enumerate(w[1:], 1):
        pieces |= {f"w{k}": a, f"e{k}": on_c(a)}

    early = place(UP_EARLY, DOWN_EARLY, (), pieces)
    up, down, bias = place(UP_LATE, DOWN_LATE, BIASES, pieces, early)
    halves = (((0, 0, 64), (64, 128, 192)), ((0, 64, 64), (64, 320, 192)))
    wholes = (((0, 0, 128),), ((0, 128, 384),))
    above0, above1 = mlp(above, wholes, up, bias, down)
    one1 = on_y(above1, 1)
    far0, far1 = mlp(far, halves, up, bias, down)
    from_below, from_above = on_y(far0, 1), on_y(far1, -1)
    below0, below1 = mlp(below, wholes, up, bias, down)
    one0 = on_y(below0, -1)
    own0, own1 = mlp([own, rest], wholes, up, bias, down, short_mlp_kernel)
    placed = []
    for h in range(2):
        sum0 = on_y(add_in(above0, from_below, h), 1)
        sum1 = on_y(add_in(below1, from_above, h), -1)
        values = (own0, own1, sum0, one0, one1, sum1, down_bias[None])
        mine, to_left, to_right, to_far = sum_up(h, *values)
        opposite = on_x(to_far, 2)
        placed += [mine, on_x(to_right, 1), on_x(to_left, -1), opposite]
    return put_out(placed)


def solution(mesh):
    grid = Mesh(mesh.devices.reshape(X, 2, 2, Y, ZH), ("x", "zl", "c", "y", "zh"))
    img, tp = ("x", "zl", "c"), ("y", "zh")
    return jax.shard_map(
        step,
        mesh=grid,
        in_specs=(P((*img, *tp), None), P(), P(), P(img, tp), P(tp), P(tp, img), P()),
        out_specs=P((*img, *tp), None),
        check_vma=False,
    )
```
